8 devices in a mesh: dp: 4 (over z, y, x), tp: 2 (over core).
Axes of the slice: x: 2, y: 2, z: 1, core: 2. Of those that a mesh axis runs over, the one named last changes fastest.
Arguments:
- w_up: bfloat16 [2, 1536, 8960], P(None, None, 'tp')
- w_down: bfloat16 [2, 8960, 1536], P(None, 'tp')
- x_saved: bfloat16 [2, 4, 4096, 1536], P(None, 'dp')
- h_saved: bfloat16 [2, 4, 4096, 8960], P(None, 'dp', None, 'tp')
- grad_out: bfloat16 [4, 4096, 1536], P('dp')
Outputs:
- output 1: bfloat16 [4, 4096, 1536], P('dp')
- output 2: float32 [2, 1536, 8960], P(None, None, 'tp')
- output 3: float32 [2, 8960, 1536], P(None, 'tp')
All inputs are finite; a program needn't handle non-finite values.
Results may differ from the reference program's by a relative error of at most 0.011775.
Values are sent between devices in bfloat16 or wider.
A program may use at most 1.25 GiB of HBM per device.

```python
import jax
import jax.numpy as jnp
from jax import lax

LAYER_COUNT = 2
BATCH_ALL = 4
SEQ_LEN = 4096
D = 1536
F = 8960


def gelu_parts(hidden):
    tanh_val = jnp.tanh(0.7978845608028654 * (hidden + 0.044715 * hidden * hidden * hidden))
    gelu_out = 0.5 * hidden * (1.0 + tanh_val)
    gelu_slope = 0.5 * (1.0 + tanh_val) + 0.5 * hidden * (1.0 - tanh_val * tanh_val) * 0.7978845608028654 * (1.0 + 0.134145 * hidden * hidden)
    return gelu_out, gelu_slope


def forward_saved(x_first, w_up, w_down):
    rows_cur = x_first.reshape(BATCH_ALL * SEQ_LEN, D)
    x_list = []
    h_list = []
    for layer_idx in range(LAYER_COUNT):
        hidden = jnp.dot(rows_cur, w_up[layer_idx], preferred_element_type=jnp.float32).astype(jnp.bfloat16)
        gelu_out = gelu_parts(hidden.astype(jnp.float32))[0]
        branch = jnp.dot(gelu_out.astype(jnp.bfloat16), w_down[layer_idx], preferred_element_type=jnp.float32)
        x_list.append(rows_cur)
        h_list.append(hidden)
        rows_cur = (rows_cur.astype(jnp.float32) + branch).astype(jnp.bfloat16)
    x_saved = jnp.stack(x_list).reshape(LAYER_COUNT, BATCH_ALL, SEQ_LEN, D)
    h_saved = jnp.stack(h_list).reshape(LAYER_COUNT, BATCH_ALL, SEQ_LEN, F)
    return x_saved, h_saved


def setup_inputs(seed: int = 0) -> dict:
    root_key = jax.random.key(seed)
    key_x, key_up, key_down, key_grad = jax.random.split(root_key, 4)
    x_first = jax.random.normal(key_x, (BATCH_ALL, SEQ_LEN, D), jnp.float32).astype(jnp.bfloat16)
    w_up = (jax.random.normal(key_up, (LAYER_COUNT, D, F), jnp.float32) * (D ** -0.5)).astype(jnp.bfloat16)
    w_down = (jax.random.normal(key_down, (LAYER_COUNT, F, D), jnp.float32) * (F ** -0.5)).astype(jnp.bfloat16)
    grad_out = jax.random.normal(key_grad, (BATCH_ALL, SEQ_LEN, D), jnp.float32).astype(jnp.bfloat16)
    x_saved, h_saved = forward_saved(x_first, w_up, w_down)
    return {"w_up": w_up, "w_down": w_down, "x_saved": x_saved, "h_saved": h_saved, "grad_out": grad_out}


def reference(w_up, w_down, x_saved, h_saved, grad_out):
    def one_sequence(accums, seq_idx):
        up_acc, down_acc = accums
        grad_cur = grad_out[seq_idx]
        up_new = [None] * LAYER_COUNT
        down_new = [None] * LAYER_COUNT
        for layer_idx in reversed(range(LAYER_COUNT)):
            x_seq = x_saved[layer_idx, seq_idx]
            gelu_out, gelu_slope = gelu_parts(h_saved[layer_idx, seq_idx].astype(jnp.float32))
            act_grad = jnp.dot(grad_cur, w_down[layer_idx].T, preferred_element_type=jnp.float32)
            hid_grad = (act_grad * gelu_slope).astype(jnp.bfloat16)
            part_sum = jnp.dot(hid_grad, w_up[layer_idx].T, preferred_element_type=jnp.float32)
            down_new[layer_idx] = jnp.dot(gelu_out.astype(jnp.bfloat16).T, grad_cur, preferred_element_type=jnp.float32)
            up_new[layer_idx] = jnp.dot(x_seq.T, hid_grad, preferred_element_type=jnp.float32)
            grad_cur = (grad_cur.astype(jnp.float32) + part_sum).astype(jnp.bfloat16)
        return (up_acc + jnp.stack(up_new), down_acc + jnp.stack(down_new)), grad_cur
    zero_acc = (jnp.zeros((LAYER_COUNT, D, F), jnp.float32), jnp.zeros((LAYER_COUNT, F, D), jnp.float32))
    (up_grad, down_grad), grad_in = lax.scan(one_sequence, zero_acc, jnp.arange(BATCH_ALL))
    return grad_in, up_grad, down_grad
```

```python
import functools

import jax
import jax.numpy as jnp
from jax import lax
from jax.experimental import pallas as pl
from jax.experimental.pallas import tpu as pltpu
from jax.sharding import PartitionSpec as P


D = 1536
F = 4480
TOKENS = 4096
QUARTER = 1120
C0 = 0.7978845608028654
NT = (((1,), (1,)), ((), ()))
VMEM_LIMIT = 67043328
ANY = pl.BlockSpec(memory_space=pl.ANY)


def gelu_pair(hidden):
    sq = hidden * hidden
    tanh_val = jnp.tanh(hidden * (C0 + (C0 * 0.044715) * sq))
    p = 0.5 + 0.5 * tanh_val
    gelu_out = hidden * p
    slope = p + (gelu_out * (1.0 - p)) * (2 * C0 + (2 * C0 * 0.134145) * sq)
    return gelu_out, slope


def dot32(a, b, dims=None):
    if dims is None:
        return jnp.dot(a, b, preferred_element_type=jnp.float32)
    return lax.dot_general(a, b, dims, preferred_element_type=jnp.float32)


def rows_of(ref, sel, start, size):
    rows = pl.ds(start, size)
    return ref.at[rows, :] if not sel else ref.at[(*sel, rows, slice(None))]


def chain_body(sub, nsub, nf, emit_w1t, g_ref, h_ref, w1_ref, w2_ref, at_ref, dht_ref, p_ref, *rest):
    w1t_ref = rest[0] if emit_w1t else None
    pacc, das, hts = rest[-3:]
    t, f = pl.program_id(0), pl.program_id(1)

    @pl.when(f == 0)
    def _():
        pacc[...] = jnp.zeros_like(pacc)

    if emit_w1t:

        @pl.when(t == 0)
        def _():
            w1t_ref[...] = w1_ref[...].T

    def first(i):
        das[i] = dot32(w2_ref[...], g_ref[pl.ds(i * sub, sub), :], NT)
        hts[i] = h_ref[pl.ds(i * sub, sub), :].T

    def second(i):
        gelu_out, slope = gelu_pair(hts[i].astype(jnp.float32))
        at_ref[:, pl.ds(i * sub, sub)] = gelu_out.astype(jnp.bfloat16)
        dht_ref[:, pl.ds(i * sub, sub)] = (das[i] * slope).astype(jnp.bfloat16)

    def third(i):
        cols = pl.ds(i * sub, sub)
        pacc[:, cols] += dot32(w1_ref[...], dht_ref[:, cols])

    first(0)
    for i in range(nsub):
        if i + 1 < nsub:
            first(i + 1)
        second(i)
        if i > 0:
            third(i - 1)
    third(nsub - 1)

    @pl.when(f == nf - 1)
    def _():
        p_ref[...] = pacc[...].T.astype(jnp.bfloat16)


def chain(grad, h_saved, w_up, w_down, layer, emit_w1t=False, fc=640, tb=1024, sub=512):
    nt, nf, nsub = TOKENS // tb, F // fc, tb // sub
    col = pl.BlockSpec((fc, tb), lambda t, f: (f, t))
    out_specs = [col, col, pl.BlockSpec((tb, D), lambda t, f: (t, 0))]
    out_shape = [(F, TOKENS), (F, TOKENS), (TOKENS, D)]
    if emit_w1t:
        out_specs.append(pl.BlockSpec((fc, D), lambda t, f: (jnp.where(t == 0, f, nf - 1), 0)))
        out_shape.append((F, D))
    return pl.pallas_call(
        functools.partial(chain_body, sub, nsub, nf, emit_w1t),
        grid=(nt, nf),
        in_specs=[
            pl.BlockSpec((tb, D), lambda t, f: (t, 0)),
            pl.BlockSpec((None, None, tb, fc), lambda t, f: (layer, 0, t, f)),
            pl.BlockSpec((None, D, fc), lambda t, f: (layer, 0, f)),
            pl.BlockSpec((None, fc, D), lambda t, f: (layer, f, 0)),
        ],
        out_specs=out_specs,
        out_shape=[jax.ShapeDtypeStruct(s, jnp.bfloat16) for s in out_shape],
        scratch_shapes=[
            pltpu.VMEM((D, tb), jnp.float32),
            pltpu.VMEM((nsub, fc, sub), jnp.float32),
            pltpu.VMEM((nsub, fc, sub), jnp.bfloat16),
        ],
        compiler_params=pltpu.CompilerParams(
            dimension_semantics=("arbitrary", "arbitrary"), vmem_limit_bytes=VMEM_LIMIT
        ),
        cost_estimate=pl.CostEstimate(flops=4 * TOKENS * D * F, bytes_accessed=6 * TOKENS * F, transcendentals=0),
    )(grad, h_saved, w_up, w_down)


def wgrad_body(cfg, *refs):
    fc, nf, tb, sub, nt = cfg["fc"], cfg["nf"], cfg["tb"], cfg["sub"], cfg["nt"]
    n_own, n_oth, srcs = cfg["n_own"], cfg["n_oth"], cfg["srcs"]
    transpose_out, layer = cfg["transpose_out"], cfg["out_layer"]
    nsub = tb // sub
    it = iter(refs)
    next(it)
    if n_own:
        at_ref, dht_ref = next(it), next(it)
    if n_oth:
        w1_ref, w2_ref = next(it), next(it)
    arrays = [next(it) for _ in range(cfg["n_arrays"])]
    acc_in = (next(it), next(it)) if cfg["acc_in"] else None
    o1, o2, xb, gb, acc1, acc2, xg_sem, in_sem, out_sem = (next(it) for _ in range(9))
    stage = next(it) if transpose_out else None
    w1t = next(it) if cfg["w1_transpose"] and n_oth else None
    if n_oth:
        hs, das, ats, dhs = (next(it) for _ in range(4))
    f, t = pl.program_id(0), pl.program_id(1)
    step = f * nt + t
    slot, fs = lax.rem(step, 2), lax.rem(f, 2)

    def start_xg(tt, sl):
        base = 0
        for xi, xsel, xrow, gi, gsel, grow, n in srcs:
            k = n // tb

            @pl.when((tt >= base) & (tt < base + k))
            def _(base=base, xi=xi, xsel=xsel, xrow=xrow, gi=gi, gsel=gsel, grow=grow):
                r = (tt - base) * tb
                xs = rows_of(arrays[xi], xsel, pl.multiple_of(xrow + r, tb), tb)
                gs = rows_of(arrays[gi], gsel, pl.multiple_of(grow + r, tb), tb)
                pltpu.make_async_copy(xs, xb.at[sl], xg_sem.at[0, sl]).start()
                pltpu.make_async_copy(gs, gb.at[sl], xg_sem.at[1, sl]).start()

            base += k

    def wait_xg(sl):
        pltpu.make_async_copy(xb.at[sl], xb.at[sl], xg_sem.at[0, sl]).wait()
        pltpu.make_async_copy(gb.at[sl], gb.at[sl], xg_sem.at[1, sl]).wait()

    def in_copies(ff, sl):
        rows = pl.ds(pl.multiple_of(ff * fc, 8), fc)
        return (
            pltpu.make_async_copy(acc_in[0].at[rows, :], acc1.at[sl], in_sem.at[0, sl]),
            pltpu.make_async_copy(acc_in[1].at[rows, :], acc2.at[sl], in_sem.at[1, sl]),
        )

    def out1(ff, sl):
        if transpose_out:
            cols = pl.ds(pl.multiple_of(ff * fc, 128), fc)
            return pltpu.make_async_copy(stage, o1.at[layer, :, cols], out_sem.at[0, 0])
        rows = pl.ds(pl.multiple_of(ff * fc, 8), fc)
        return pltpu.make_async_copy(acc1.at[sl], o1.at[rows, :], out_sem.at[0, sl])

    def out2(ff, sl):
        rows = pl.ds(pl.multiple_of(ff * fc, 8), fc)
        dst = o2.at[rows, :] if layer is None else o2.at[layer, rows, :]
        return pltpu.make_async_copy(acc2.at[sl], dst, out_sem.at[1, sl])

    def wait_out(ff, sl):
        out2(ff, sl).wait()
        if not transpose_out:
            out1(ff, sl).wait()

    @pl.when(step == 0)
    def _():
        start_xg(jnp.int32(0), 0)
        if acc_in is not None:
            for c in in_copies(0, 0):
                c.start()

    @pl.when(step + 1 < nf * nt)
    def _():
        start_xg(jnp.where(t + 1 == nt, 0, t + 1), 1 - slot)

    @pl.when(t == 0)
    def _():
        if acc_in is not None:
            for c in in_copies(f, fs):
                c.wait()
        else:

            @pl.when(f >= 2)
            def _():
                wait_out(f - 2, fs)

            acc1[fs] = jnp.zeros((fc, D), jnp.float32)
            acc2[fs] = jnp.zeros((fc, D), jnp.float32)
        if w1t is not None:
            w1t[...] = w1_ref[...].T

    if acc_in is not None:

        @pl.when((t == 1) & (f + 1 < nf))
        def _():
            @pl.when(f >= 1)
            def _():
                wait_out(f - 1, 1 - fs)

            for c in in_copies(f + 1, 1 - fs):
                c.start()

    wait_xg(slot)

    if n_own:

        @pl.when(t < n_own)
        def _():
            acc2[fs] += dot32(at_ref[...], gb[slot])
            acc1[fs] += dot32(dht_ref[...], xb[slot])

    if n_oth:

        @pl.when(t >= n_own)
        def _():
            left1 = w1t if w1t is not None else w1_ref

            def first(i):
                hs[i] = dot32(left1[...], xb[slot, pl.ds(i * sub, sub), :], NT)
                das[i] = dot32(w2_ref[...], gb[slot, pl.ds(i * sub, sub), :], NT)

            def second(i):
                gelu_out, slope = gelu_pair(hs[i].astype(jnp.bfloat16).astype(jnp.float32))
                ats[i] = gelu_out.astype(jnp.bfloat16)
                dhs[i] = (das[i] * slope).astype(jnp.bfloat16)

            def third(i):
                acc2[fs] += dot32(ats[i], gb[slot, pl.ds(i * sub, sub), :])
                acc1[fs] += dot32(dhs[i], xb[slot, pl.ds(i * sub, sub), :])

            first(0)
            for i in range(nsub):
                if i + 1 < nsub:
                    first(i + 1)
                second(i)
                if i > 0:
                    third(i - 1)
            third(nsub - 1)

    @pl.when(t == nt - 1)
    def _():
        if transpose_out:

            @pl.when(f >= 1)
            def _():
                out1(f - 1, 1 - fs).wait()

            stage[...] = acc1[fs].T
        out1(f, fs).start()
        out2(f, fs).start()

        @pl.when(f == nf - 1)
        def _():
            out1(f, fs).wait()
            out2(f, fs).wait()
            if nf > 1:
                wait_out(f - 1, 1 - fs)


def wgrad(
    q, w1, w2, layer, rows, fc, *, own=None, own_sources=(), sources=(), acc_in=None, tb=1024, sub=512,
    transpose_out=False, w1_transpose=False, out_layer=None, block_mul=0,
):
    nf = rows // fc
    arrays, srcs = [], []

    def index_of(arr):
        for i, known in enumerate(arrays):
            if known is arr:
                return i
        arrays.append(arr)
        return len(arrays) - 1

    for x, xsel, xrow, g, gsel, grow, n in (*own_sources, *sources):
        srcs.append((index_of(x), xsel, xrow, index_of(g), gsel, grow, n))
    n_own = sum(s[-1] for s in own_sources) // tb
    n_oth = sum(s[-1] for s in sources) // tb
    nt = n_own + n_oth
    cfg = dict(
        fc=fc, nf=nf, tb=tb, sub=sub, nt=nt, n_own=n_own, n_oth=n_oth, srcs=srcs, n_arrays=len(arrays),
        acc_in=acc_in is not None, transpose_out=transpose_out, w1_transpose=w1_transpose, out_layer=out_layer,
    )
    block = (lambda f, q_ref: f + block_mul * q_ref[0]) if block_mul else (lambda f, q_ref: f)
    ins, in_specs = [], []
    if n_own:
        spec = pl.BlockSpec((fc, tb), lambda f, t, q_ref: (block(f, q_ref), jnp.minimum(t, n_own - 1)))
        ins += list(own)
        in_specs += [spec, spec]
    if n_oth:
        if w1_transpose:
            in_specs.append(pl.BlockSpec((None, D, fc), lambda f, t, q_ref: (layer, 0, block(f, q_ref))))
        else:
            in_specs.append(pl.BlockSpec((fc, D), lambda f, t, q_ref: (block(f, q_ref), 0)))
        in_specs.append(pl.BlockSpec((None, fc, D), lambda f, t, q_ref: (layer, block(f, q_ref), 0)))
        ins += [w1, w2]
    ins += arrays
    if acc_in is not None:
        ins += list(acc_in)
    in_specs += [ANY] * (len(ins) - len(in_specs))
    scratch = [
        pltpu.VMEM((2, tb, D), jnp.bfloat16),
        pltpu.VMEM((2, tb, D), jnp.bfloat16),
        pltpu.VMEM((2, fc, D), jnp.float32),
        pltpu.VMEM((2, fc, D), jnp.float32),
        pltpu.SemaphoreType.DMA((2, 2)),
        pltpu.SemaphoreType.DMA((2, 2)),
        pltpu.SemaphoreType.DMA((2, 2)),
    ]
    if transpose_out:
        scratch.append(pltpu.VMEM((D, fc), jnp.float32))
    if w1_transpose and n_oth:
        scratch.append(pltpu.VMEM((fc, D), jnp.bfloat16))
    if n_oth:
        nsub = tb // sub
        scratch += [pltpu.VMEM((nsub, fc, sub), jnp.float32)] * 2
        scratch += [pltpu.VMEM((nsub, fc, sub), jnp.bfloat16)] * 2
    if transpose_out:
        shapes = [(2, D, F), (2, F, D)]
    else:
        shapes = [(rows, D), (rows, D)]
    flops = 4 * tb * (n_own + 2 * n_oth) * D * rows
    return pl.pallas_call(
        functools.partial(wgrad_body, cfg),
        grid_spec=pltpu.PrefetchScalarGridSpec(
            num_scalar_prefetch=1, grid=(nf, nt), in_specs=in_specs, out_specs=[ANY] * 2, scratch_shapes=scratch
        ),
        out_shape=[jax.ShapeDtypeStruct(s, jnp.float32) for s in shapes],
        compiler_params=pltpu.CompilerParams(
            dimension_semantics=("arbitrary", "arbitrary"), vmem_limit_bytes=VMEM_LIMIT
        ),
        cost_estimate=pl.CostEstimate(flops=flops, bytes_accessed=16 * rows * D, transcendentals=0),
    )(q, *ins)


def place_body(q_ref, *refs):
    ones, twos = refs[0:4], refs[4:8]
    o1, o2, buf, slots, stage, in_sem, two_in, two_out, out_sem = refs[10:]
    q = q_ref[0]
    fc = stage.shape[2]

    def rows(k):
        return pl.ds(pl.multiple_of(jnp.bitwise_xor(q, k) * QUARTER, 8), QUARTER)

    first = [pltpu.make_async_copy(ones[k], buf.at[rows(k), :], in_sem.at[k]) for k in range(4)]
    for c in first:
        c.start()
    two = [pltpu.make_async_copy(twos[k], slots.at[k % 2], two_in.at[k % 2]) for k in range(4)]
    out = [pltpu.make_async_copy(slots.at[k % 2], o2.at[0, rows(k), :], two_out.at[k % 2]) for k in range(4)]
    two[0].start()
    two[1].start()
    for c in first:
        c.wait()
    done = [
        pltpu.make_async_copy(stage.at[j % 2], o1.at[0, :, pl.ds(j * fc, fc)], out_sem.at[j % 2])
        for j in range(F // fc)
    ]
    for j in range(F // fc):
        if j >= 2:
            done[j - 2].wait()
        stage[j % 2] = buf[pl.ds(j * fc, fc), :].T
        done[j].start()
        if j < 4:
            two[j].wait()
            out[j].start()
            if j >= 1 and j + 1 < 4:
                out[j - 1].wait()
                two[j + 1].start()
    for c in (out[2], out[3], *done[-2:]):
        c.wait()


def place(q, ones, twos, dest):
    return pl.pallas_call(
        place_body,
        grid_spec=pltpu.PrefetchScalarGridSpec(
            num_scalar_prefetch=1,
            grid=(1,),
            in_specs=[ANY] * 10,
            out_specs=[ANY] * 2,
            scratch_shapes=[
                pltpu.VMEM((F, D), jnp.float32),
                pltpu.VMEM((2, QUARTER, D), jnp.float32),
                pltpu.VMEM((2, D, 640), jnp.float32),
                pltpu.SemaphoreType.DMA((4,)),
                pltpu.SemaphoreType.DMA((2,)),
                pltpu.SemaphoreType.DMA((2,)),
                pltpu.SemaphoreType.DMA((2,)),
            ],
        ),
        out_shape=[jax.ShapeDtypeStruct((2, D, F), jnp.float32), jax.ShapeDtypeStruct((2, F, D), jnp.float32)],
        input_output_aliases={9: 0, 10: 1},
        compiler_params=pltpu.CompilerParams(dimension_semantics=("arbitrary",), vmem_limit_bytes=VMEM_LIMIT),
        cost_estimate=pl.CostEstimate(flops=10**9, bytes_accessed=16 * F * D, transcendentals=0),
        name="place",
    )(q, *ones, *twos, *dest)


X_PERM = [(i, i ^ 1) for i in range(4)]
Y_PERM = [(i, i ^ 2) for i in range(4)]
C_PERM = [(0, 1), (1, 0)]


def over_x(a):
    return lax.ppermute(a, "dp", X_PERM)


def over_y(a):
    return lax.ppermute(a, "dp", Y_PERM)


def over_c(a):
    return lax.ppermute(a, "tp", C_PERM)


def after(value, *before):
    return lax.optimization_barrier((value, *before))[0]


def add_parts(grad, own, other):
    total = own.astype(jnp.float32) + other.astype(jnp.float32)
    return (grad.astype(jnp.float32) + total).astype(jnp.bfloat16)


def solution(mesh):
    def backward(w_up, w_down, x_saved, h_saved, grad_out):
        core = lax.axis_index("tp")
        chip = lax.axis_index("dp")
        q_keep = chip.astype(jnp.int32).reshape(1)
        q_send = jnp.bitwise_xor(q_keep, 2)
        zero = jnp.zeros((1,), jnp.int32)

        grad = grad_out[0]

        def half(a, *sel):
            start = (*sel, core * 2048, 0)
            return lax.dynamic_slice(a, start, (1,) * len(sel) + (2048, D)).reshape(2048, D)

        g2h, x0h, x1h = half(grad_out, 0), half(x_saved, 0, 0), half(x_saved, 1, 0)
        g2y, x0x = over_y(g2h), over_x(x0h)
        x1y = over_y(x1h)

        aT1, dHT1, p1 = chain(after(grad, g2h, x0h, x1h), h_saved, w_up, w_down, 1)
        g1 = add_parts(grad, p1, over_c(p1))
        g1h = half(g1)
        g1x = over_x(g1h)
        g2x, x1x = over_x(after(g2h, g1h)), over_x(after(x1h, g1h))
        g2d, x1d = over_y(g2x), over_x(x1y)
        x0x_c, g1x_c = over_c(x0x), over_c(g1x)
        g2y_c, x1y_c = over_c(g2y), over_c(x1y)
        g2x_c, x1x_c = over_c(g2x), over_c(x1x)
        g2d_c, x1d_c = over_c(g2d), over_c(x1d)

        aT0, dHT0, p0, w1t0 = chain(after(g1, g1h), h_saved, w_up, w_down, 0, emit_w1t=True)
        p0_c = over_c(p0)

        own0 = dict(
            own=(aT0, dHT0),
            own_sources=[(x_saved, (0, 0), 0, g1, (), 0, TOKENS)],
            sources=[(x0x, (), 0, g1x, (), 0, 2048), (x0x_c, (), 0, g1x_c, (), 0, 2048)],
            block_mul=2,
        )
        s1, s2 = wgrad(q_send, w1t0, w_down, 0, QUARTER, 560, **own0)
        r1, r2 = over_y(s1), over_y(s2)

        part = wgrad(
            after(zero, s1), w_up, w_down, 1, F, 640, w1_transpose=True, own=(aT1, dHT1),
            own_sources=[(x_saved, (1, 0), 0, grad_out, (0,), 0, TOKENS)],
            sources=[(x1y, (), 0, g2y, (), 0, 2048), (x1y_c, (), 0, g2y_c, (), 0, 2048)],
        )
        f1, f2 = wgrad(after(q_keep, part[0]), w1t0, w_down, 0, QUARTER, 560, acc_in=(r1, r2), **own0)
        f1x, f2y = over_x(f1), over_y(f2)
        f2x, f1y = over_x(f2), over_y(f1)
        f1d, f2d = over_y(f1x), over_x(f2y)
        part = wgrad(
            after(zero, f1), w_up, w_down, 1, F, 640, acc_in=part, w1_transpose=True,
            sources=[(x1x, (), 0, g2x, (), 0, 2048), (x1x_c, (), 0, g2x_c, (), 0, 2048)],
        )
        g0 = add_parts(g1, after(p0, part[0]), p0_c)
        dest = wgrad(
            after(zero, part[0]), w_up, w_down, 1, F, 640, acc_in=part, w1_transpose=True, transpose_out=True,
            out_layer=1,
            sources=[(x1d, (), 0, g2d, (), 0, 2048), (x1d_c, (), 0, g2d_c, (), 0, 2048)],
        )
        up, down = place(q_keep, (f1, f1x, f1y, f1d), (f2, f2x, f2y, f2d), dest)
        return g0[None], up, down

    return jax.shard_map(
        backward,
        mesh=mesh,
        in_specs=(
            P(None, None, "tp"),
            P(None, "tp", None),
            P(None, "dp", None, None),
            P(None, "dp", None, "tp"),
            P("dp", None, None),
        ),
        out_specs=(P("dp", None, None), P(None, None, "tp"), P(None, "tp", None)),
        check_vma=False,
    )
```
